32 devices in a mesh: rep: 1, dp: 32 (over x, y, z, core).
Axes of the slice: x: 2, y: 2, z: 4, core: 2. Of those that a mesh axis runs over, the one named last changes fastest.
Arguments:
- x: bfloat16 [32, 2048, 768], P(('rep', 'dp'))
- dy: bfloat16 [32, 2048, 768], P(('rep', 'dp'))
- wq: bfloat16 [2, 768, 768], P(None, 'dp')
- wk: bfloat16 [2, 768, 256], P(None, 'dp')
- wv: bfloat16 [2, 768, 256], P(None, 'dp')
- wo: bfloat16 [2, 768, 768], P(None, 'dp')
- w_gate: bfloat16 [2, 768, 2048], P(None, 'dp')
- w_up: bfloat16 [2, 768, 2048], P(None, 'dp')
- w_down: bfloat16 [2, 2048, 768], P(None, 'dp')
- m_wq: float32 [2, 768, 768], P(None, 'dp')
- m_wk: float32 [2, 768, 256], P(None, 'dp')
- m_wv: float32 [2, 768, 256], P(None, 'dp')
- m_wo: float32 [2, 768, 768], P(None, 'dp')
- m_w_gate: float32 [2, 768, 2048], P(None, 'dp')
- m_w_up: float32 [2, 768, 2048], P(None, 'dp')
- m_w_down: float32 [2, 2048, 768], P(None, 'dp')
- v_wq: float32 [2, 768, 768], P(None, 'dp')
- v_wk: float32 [2, 768, 256], P(None, 'dp')
- v_wv: float32 [2, 768, 256], P(None, 'dp')
- v_wo: float32 [2, 768, 768], P(None, 'dp')
- v_w_gate: float32 [2, 768, 2048], P(None, 'dp')
- v_w_up: float32 [2, 768, 2048], P(None, 'dp')
- v_w_down: float32 [2, 2048, 768], P(None, 'dp')
Outputs:
- output 1: bfloat16 [2, 768, 768], P('rep', 'dp')
- output 2: bfloat16 [2, 768, 256], P('rep', 'dp')
- output 3: bfloat16 [2, 768, 256], P('rep', 'dp')
- output 4: bfloat16 [2, 768, 768], P('rep', 'dp')
- output 5: bfloat16 [2, 768, 2048], P('rep', 'dp')
- output 6: bfloat16 [2, 768, 2048], P('rep', 'dp')
- output 7: bfloat16 [2, 2048, 768], P('rep', 'dp')
- output 8: float32 [2, 768, 768], P('rep', 'dp')
- output 9: float32 [2, 768, 256], P('rep', 'dp')
- output 10: float32 [2, 768, 256], P('rep', 'dp')
- output 11: float32 [2, 768, 768], P('rep', 'dp')
- output 12: float32 [2, 768, 2048], P('rep', 'dp')
- output 13: float32 [2, 768, 2048], P('rep', 'dp')
- output 14: float32 [2, 2048, 768], P('rep', 'dp')
- output 15: float32 [2, 768, 768], P('rep', 'dp')
- output 16: float32 [2, 768, 256], P('rep', 'dp')
- output 17: float32 [2, 768, 256], P('rep', 'dp')
- output 18: float32 [2, 768, 768], P('rep', 'dp')
- output 19: float32 [2, 768, 2048], P('rep', 'dp')
- output 20: float32 [2, 768, 2048], P('rep', 'dp')
- output 21: float32 [2, 2048, 768], P('rep', 'dp')
All inputs are finite; a program needn't handle non-finite values.
Results may differ from the reference program's by a relative error of at most 0.024.
Values are sent between devices in bfloat16 or wider.
A program may use at most 2 GiB of HBM per device.

```python
import jax
import jax.numpy as jnp
from jax import lax

SEQUENCES = 32
TOKENS = 2048
D = 768
HEADS = 6
KV_HEADS = 2
HEAD = 128
FF = 2048
LAYERS = 2
THETA = 10000
NAMES = ("wq", "wk", "wv", "wo", "w_gate", "w_up", "w_down")
SHAPES = {
    "wq": (LAYERS, D, HEADS * HEAD),
    "wk": (LAYERS, D, KV_HEADS * HEAD),
    "wv": (LAYERS, D, KV_HEADS * HEAD),
    "wo": (LAYERS, HEADS * HEAD, D),
    "w_gate": (LAYERS, D, FF),
    "w_up": (LAYERS, D, FF),
    "w_down": (LAYERS, FF, D),
}


def bump(key, n, height):
    away = (jnp.arange(n, dtype=jnp.int32) - jax.random.randint(key, (), 0, n, jnp.int32)) % n
    return jnp.where(away < n // 8, height, 1.0)


def together(key, own, strength):
    shared = jax.random.normal(key, own.shape[1:], jnp.float32)
    return (own + strength * shared) * lax.rsqrt(1 + strength * strength)


def setup_inputs(seed: int = 0, part: int = 0) -> dict:
    kx, kdy, ka, kb, kz, kf, kh, kl, *keys = jax.random.split(jax.random.key(seed), 8 + 3 * len(NAMES))
    kx, kdy, ka, kb = (jax.random.fold_in(k, part) for k in (kx, kdy, ka, kb))
    kw, km, kv = (keys[i::3] for i in range(3))
    shape = (SEQUENCES, TOKENS, D)
    much_x, much_dy = jax.random.uniform(kz, (2,), jnp.float32, 0.0, 1.0)
    loud = 2.0 ** jax.random.uniform(jax.random.fold_in(kz, 1), (), jnp.float32, -1.0, 2.0)
    layers = 2.0 ** jax.random.uniform(kl, (LAYERS, 1, 1), jnp.float32, -1.0, 1.0)
    times = {"wq": 1.0, "wk": 1.0, "wv": 2.0, "wo": layers, "w_gate": 1.0, "w_up": bump(kh, FF, 4.0), "w_down": layers}
    x = together(ka, jax.random.normal(kx, shape, jnp.float32), much_x) * bump(kf, D, 4.0)
    dy = together(kb, jax.random.normal(kdy, shape, jnp.float32), much_dy)
    drawn = {"x": x.astype(jnp.bfloat16), "dy": (loud * dy * (SEQUENCES * TOKENS) ** -0.5).astype(jnp.bfloat16)}
    for key, name in zip(kw, NAMES, strict=True):
        drawn[name] = (jax.random.normal(key, SHAPES[name], jnp.float32) * SHAPES[name][1] ** -0.5 * times[name]).astype(jnp.bfloat16)
    for key, name in zip(km, NAMES, strict=True):
        drawn[f"m_{name}"] = 0.1 * jax.random.normal(key, SHAPES[name], jnp.float32)
    for key, name in zip(kv, NAMES, strict=True):
        drawn[f"v_{name}"] = jax.random.uniform(key, SHAPES[name], jnp.float32, 0.02, 0.06)
    return drawn


def matmul(a, w):
    return jnp.dot(a, w, preferred_element_type=jnp.float32).astype(jnp.bfloat16)


def normed(h):
    wide = h.astype(jnp.float32)
    scale = lax.rsqrt(jnp.mean(wide**2, -1, keepdims=True) + 1e-6)
    return (wide * scale).astype(jnp.bfloat16)


def turned(t, theta):
    half = t.shape[-1] // 2
    angle = jnp.arange(t.shape[0], dtype=jnp.float32)[:, None] * theta ** (-jnp.arange(half, dtype=jnp.float32) / half)
    cos, sin = jnp.cos(angle)[:, None], jnp.sin(angle)[:, None]
    a, b = t[..., :half].astype(jnp.float32), t[..., half:].astype(jnp.float32)
    return jnp.concatenate([a * cos - b * sin, b * cos + a * sin], -1).astype(jnp.bfloat16)


def seen_by(q, k, v):
    tokens, kv = q.shape[0], k.shape[1]
    q = q.reshape(tokens, kv, -1, q.shape[-1])
    scores = jnp.einsum("tgsd,ugd->gstu", q.astype(jnp.float32), k.astype(jnp.float32)) * q.shape[-1] ** -0.5
    place = jnp.arange(tokens)
    weights = jax.nn.softmax(jnp.where(place[:, None] >= place, scores, -jnp.inf), -1).astype(jnp.bfloat16)
    return jnp.einsum("gstu,ugd->tgsd", weights.astype(jnp.float32), v.astype(jnp.float32)).astype(jnp.bfloat16).reshape(tokens, -1)


def layer(h, w):
    a = normed(h)
    q, k = (turned(matmul(a, w[name]).reshape(h.shape[0], -1, HEAD), THETA) for name in ("wq", "wk"))
    h = h + matmul(seen_by(q, k, matmul(a, w["wv"]).reshape(h.shape[0], -1, HEAD)), w["wo"])
    b = normed(h)
    gate = jnp.dot(b, w["w_gate"], preferred_element_type=jnp.float32)
    up = jnp.dot(b, w["w_up"], preferred_element_type=jnp.float32)
    return h + matmul((jax.nn.silu(gate) * up).astype(jnp.bfloat16), w["w_down"])


def adamw(w, m, v, g):
    m = 0.9 * m + 0.1 * g
    v = 0.95 * v + 0.05 * g * g
    step = m * lax.rsqrt(v + 1e-8) + 0.1 * w
    return (w - 0.02 * step).astype(jnp.bfloat16), m, v


def clipped(gradients, sum_of_squares, count):
    factor = jnp.minimum(1.0, 0.5 * lax.rsqrt(sum_of_squares / count + 1e-30))
    return [g * factor for g in gradients]


def stack(weights, h):
    return lax.scan(lambda h, w: (layer(h, w), None), h, weights)[0]


def reference(x, dy, wq, wk, wv, wo, w_gate, w_up, w_down, m_wq, m_wk, m_wv, m_wo, m_w_gate, m_w_up, m_w_down, v_wq, v_wk, v_wv, v_wo, v_w_gate, v_w_up, v_w_down):
    weights = dict(zip(NAMES, (wq, wk, wv, wo, w_gate, w_up, w_down), strict=True))

    def take(so_far, sequence):
        h, by_y = sequence
        _, back = jax.vjp(stack, weights, h)
        by_weights, by_h = back(by_y)
        return jax.tree.map(lambda total, term: total + term.astype(jnp.float32), so_far, by_weights), by_h

    none_yet = {name: jnp.zeros(w.shape, jnp.float32) for name, w in weights.items()}
    by_weights, by_x = lax.scan(take, none_yet, (x, dy))
    gradients = [by_weights[name].astype(jnp.bfloat16).astype(jnp.float32) for name in NAMES]
    gradients = clipped(gradients, sum(jnp.sum(g * g) for g in gradients), sum(g.size for g in gradients))
    first = (m_wq, m_wk, m_wv, m_wo, m_w_gate, m_w_up, m_w_down)
    second = (v_wq, v_wk, v_wv, v_wo, v_w_gate, v_w_up, v_w_down)
    new = [adamw(weights[name].astype(jnp.float32), m, v, g) for name, m, v, g in zip(NAMES, first, second, gradients, strict=True)]
    return tuple(one[which] for which in range(3) for one in new)
```

```python
import functools

import jax, jax.numpy as jnp
from jax import lax
from jax.experimental import pallas as pl
from jax.experimental.pallas import tpu as pltpu
F32, BF = jnp.float32, jnp.bfloat16
D, FF, HEAD, QH, KVH = 768, 2048, 128, 6, 2
VM = 60*2**20

def dot(a, b, ca=1, cb=0):
    return lax.dot_general(a, b, (((ca,), (cb,)), ((), ())), preferred_element_type=F32)

def _norm(h):
    wide = h.astype(F32)
    return wide * lax.rsqrt(jnp.mean(wide * wide, -1, keepdims=True) + 1e-6)

def _norm_back(h, g):
    wide = h.astype(F32)
    scale = lax.rsqrt(jnp.mean(wide * wide, -1, keepdims=True) + 1e-6)
    inner = jnp.mean(g * wide, -1, keepdims=True)
    return scale * g - wide * (scale * scale * scale * inner)

def _turn(t, c, s):
    return t * c + pltpu.roll(t, 64, 1) * s

def rows(n, w): return pl.BlockSpec((n, w), lambda i: (i, 0))
def heads(n, bt): return pl.BlockSpec((n, bt, HEAD), lambda i: (0, i, 0))
def whole(shape, *at): return pl.BlockSpec(shape, lambda i: at, pipeline_mode=pl.Buffered(1))
def params(sem="arbitrary"): return pltpu.CompilerParams(dimension_semantics=(sem,), vmem_limit_bytes=VM)
def cost(flops, nbytes): return pl.CostEstimate(flops=int(flops), bytes_accessed=int(nbytes), transcendentals=0)
def sds(shape, dt=BF): return jax.ShapeDtypeStruct(shape, dt)

def _qkv(h_ref, wq_ref, wkv_ref, c_ref, s_ref, q_ref, k_ref, v_ref):
    a = _norm(h_ref[...]).astype(BF)
    c, s = c_ref[...], s_ref[...]
    q = dot(a, wq_ref[...]).astype(BF)
    for n in range(QH):
        q_ref[n] = _turn(q[:, n*HEAD:(n+1)*HEAD].astype(F32), c, s).astype(BF)
    kv = dot(a, wkv_ref[...]).astype(BF)
    for n in range(KVH):
        k_ref[n] = _turn(kv[:, n*HEAD:(n+1)*HEAD].astype(F32), c, s).astype(BF)
        v_ref[n] = kv[:, (KVH+n)*HEAD:(KVH+n+1)*HEAD]

def qkv(h, narrow, c, s, bt=512):
    T = h.shape[0]
    return pl.pallas_call(_qkv, grid=(T//bt,),
        in_specs=[rows(bt, D), whole((D, 768), 0, 0), whole((D, 512), 0, 3), rows(bt, HEAD), rows(bt, HEAD)],
        out_specs=[heads(QH, bt), heads(KVH, bt), heads(KVH, bt)],
        out_shape=[sds((QH, T, HEAD)), sds((KVH, T, HEAD)), sds((KVH, T, HEAD))],
        compiler_params=params(), cost_estimate=cost(2*T*D*1280, 12e6))(h, narrow, narrow, c, s)

def _mlp(h_ref, o_ref, wo_ref, wg_ref, wu_ref, wd_ref, hm_ref, gate_ref, up_ref, out_ref, prod_s, *, chunk):
    hm = (h_ref[...].astype(F32) + dot(o_ref[...], wo_ref[...]).astype(BF).astype(F32)).astype(BF)
    hm_ref[...] = hm
    b = _norm(hm).astype(BF)
    for at in range(0, FF, chunk):
        cut = slice(at, at+chunk)
        gate = dot(b, wg_ref[:, cut]); up = dot(b, wu_ref[:, cut])
        gate_ref[:, cut] = gate; up_ref[:, cut] = up
        prod_s[:, cut] = (gate * lax.logistic(gate) * up).astype(BF)
    out_ref[...] = (hm.astype(F32) + dot(prod_s[...], wd_ref[...]).astype(BF).astype(F32)).astype(BF)

def mlp(h, o, narrow, wg, wu, wd, bt=256, chunk=512):
    T = h.shape[0]
    return pl.pallas_call(functools.partial(_mlp, chunk=chunk), grid=(T//bt,),
        in_specs=[rows(bt, D), rows(bt, D), whole((D, 768), 0, 1), whole((D, FF), 0, 0), whole((D, FF), 0, 0), whole((FF, D), 0, 0)],
        out_specs=[rows(bt, D), rows(bt, FF), rows(bt, FF), rows(bt, D)],
        out_shape=[sds((T, D)), sds((T, FF), F32), sds((T, FF), F32), sds((T, D))],
        scratch_shapes=[pltpu.VMEM((bt, FF), BF)],
        compiler_params=params(), cost_estimate=cost(2*T*D*(768+3*FF), 60e6))(h, o, narrow, wg, wu, wd)

def _mlp_back(dy_ref, gate_ref, up_ref, hm_ref, o_ref, wg_ref, wu_ref, wd_ref, wo_ref, dhm_ref, dgate_ref, dup_ref, prod_ref, do_ref, delta_ref, *, chunk):
    dy = dy_ref[...]
    for at in range(0, FF, chunk):
        cut = slice(at, at+chunk)
        dprod = dot(dy, wd_ref[cut, :], 1, 1).astype(BF).astype(F32)
        gate, up = gate_ref[:, cut], up_ref[:, cut]
        sig = lax.logistic(gate)
        act = gate * sig
        prod_ref[:, cut] = (act * up).astype(BF)
        dup_ref[:, cut] = (dprod * act).astype(BF)
        dgate_ref[:, cut] = (dprod * up * (sig + act * (1 - sig))).astype(BF)
    db = (dot(dgate_ref[...], wg_ref[...], 1, 1) + dot(dup_ref[...], wu_ref[...], 1, 1)).astype(BF).astype(F32)
    dhm = (dy.astype(F32) + _norm_back(hm_ref[...], db).astype(BF).astype(F32)).astype(BF)
    dhm_ref[...] = dhm
    do = dot(dhm, wo_ref[...], 1, 1).astype(BF)
    both = do.astype(F32) * o_ref[...].astype(F32)
    for n in range(QH):
        at = slice(n*HEAD, (n+1)*HEAD)
        do_ref[n] = do[:, at]
        delta_ref[n:n+1, :] = jnp.sum(both[:, at].T, axis=0, keepdims=True)

def mlp_back(dy, gate, up, hm, o, narrow, wg, wu, wd, bt=256, chunk=512):
    T = dy.shape[0]
    return pl.pallas_call(functools.partial(_mlp_back, chunk=chunk), grid=(T//bt,),
        in_specs=[rows(bt, D), rows(bt, FF), rows(bt, FF), rows(bt, D), rows(bt, D), whole((D, FF), 0, 0), whole((D, FF), 0, 0), whole((FF, D), 0, 0), whole((D, 768), 0, 1)],
        out_specs=[rows(bt, D), rows(bt, FF), rows(bt, FF), rows(bt, FF), heads(QH, bt), pl.BlockSpec((QH, bt), lambda i: (0, i))],
        out_shape=[sds((T, D)), sds((T, FF)), sds((T, FF)), sds((T, FF)), sds((QH, T, HEAD)), sds((QH, T), F32)],
        compiler_params=params(), cost_estimate=cost(2*T*D*(768+3*FF), 80e6))(dy, gate, up, hm, o, wg, wu, wd, narrow)

def _mlp_wgrad(hm_ref, dy_ref, dgate_ref, dup_ref, prod_ref, wg_ref, wu_ref, wd_ref, b_s, dy_s):
    @pl.when(pl.program_id(0) == 0)
    def _():
        b_s[...] = _norm(hm_ref[...]).astype(BF)
    wg_ref[...] = dot(b_s[...], dgate_ref[...], 0, 0).astype(BF)
    wu_ref[...] = dot(b_s[...], dup_ref[...], 0, 0).astype(BF)
    wd_ref[...] = dot(prod_ref[...], dy_ref[...], 0, 0).astype(BF)

def mlp_wgrad(hm, dy, dgate, dup, prod, cw=512):
    T = dy.shape[0]
    cols = lambda n: pl.BlockSpec((n, cw), lambda i: (0, i))
    return pl.pallas_call(_mlp_wgrad, grid=(FF//cw,),
        in_specs=[whole((T, D), 0, 0), whole((T, D), 0, 0), cols(T), cols(T), cols(T)],
        out_specs=[cols(D), cols(D), rows(cw, D)],
        out_shape=[sds((D, FF)), sds((D, FF)), sds((FF, D))],
        scratch_shapes=[pltpu.VMEM((T, D), BF), pltpu.VMEM((T, D), BF)],
        compiler_params=params(), cost_estimate=cost(6*T*D*FF, 40e6))(hm, dy, dgate, dup, prod)

def _qkv_back(dq_ref, dk_ref, dv_ref, c_ref, s_ref, h_ref, dhm_ref, wq_ref, wkv_ref, dqkv_ref, dh_ref):
    c, s = c_ref[...], s_ref[...]
    for n in range(QH + KVH):
        t = (dq_ref[n] if n < QH else dk_ref[n-QH]).astype(F32)
        dqkv_ref[:, n*HEAD:(n+1)*HEAD] = _turn(t, c, -s).astype(BF)
    for n in range(KVH):
        dqkv_ref[:, (QH+KVH+n)*HEAD:(QH+KVH+n+1)*HEAD] = dv_ref[n]
    if dh_ref is not None:
        da = (dot(dqkv_ref[:, :768], wq_ref[...], 1, 1) + dot(dqkv_ref[:, 768:], wkv_ref[...], 1, 1)).astype(BF).astype(F32)
        dh_ref[...] = (dhm_ref[...].astype(F32) + _norm_back(h_ref[...], da).astype(BF).astype(F32)).astype(BF)

def qkv_back(dq, dk, dv, c, s, h, dhm, narrow, bt=512):
    T = h.shape[0]
    return pl.pallas_call(_qkv_back, grid=(T//bt,),
        in_specs=[heads(QH, bt), heads(KVH, bt), heads(KVH, bt), rows(bt, HEAD), rows(bt, HEAD), rows(bt, D), rows(bt, D), whole((D, 768), 0, 0), whole((D, 512), 0, 3)],
        out_specs=[rows(bt, 1280), rows(bt, D)],
        out_shape=[sds((T, 1280)), sds((T, D))],
        compiler_params=params(), cost_estimate=cost(2*T*D*1280, 20e6))(dq, dk, dv, c, s, h, dhm, narrow, narrow)

def _attn_wgrad(h_ref, o_ref, dhm_ref, dqkv_ref, out_ref):
    a = _norm(h_ref[...]).astype(BF)
    g = dot(a, dqkv_ref[...], 0, 0).astype(BF)
    out_ref[:, :768] = g[:, :768]
    out_ref[:, 1536:] = g[:, 768:]
    out_ref[:, 768:1536] = dot(o_ref[...], dhm_ref[...], 0, 0).astype(BF)

def attn_wgrad(h, o, dhm, dqkv, bm=256):
    T = h.shape[0]
    full = lambda w: pl.BlockSpec((T, w), lambda i: (0, 0), pipeline_mode=pl.Buffered(1))
    return pl.pallas_call(_attn_wgrad, grid=(1,),
        in_specs=[full(D), full(D), full(D), full(1280)],
        out_specs=pl.BlockSpec((D, FF), lambda i: (0, 0)),
        out_shape=sds((D, FF)),
        compiler_params=params(), cost_estimate=cost(2*T*D*FF, 20e6))(h, o, dhm, dqkv)

LOG2E = 1.4426950408889634
NEG = -1e30
SCALE = HEAD ** -0.5
G = QH // KVH

def _order(rows_, cols_):
    return lax.broadcasted_iota(jnp.int32, (rows_, cols_), 1) >= lax.broadcasted_iota(jnp.int32, (rows_, cols_), 0)

def _strips(bq, half):
    return [(at, half, at) for at in range(0, bq, half)]

def _attend(q_ref, k_ref, v_ref, o_ref, lse_ref, top_s, mix_s, vt_s, *, bq, bk, half):
    iq = pl.program_id(0)
    e = SCALE * LOG2E

    @pl.when(iq == 0)
    def _():
        for i in range(KVH):
            vt_s[i, :HEAD, :] = v_ref[i].T
            vt_s[i, HEAD:, :] = jnp.ones((16, v_ref.shape[1]), BF)

    top_s[...] = jnp.full(top_s.shape, NEG, F32)
    mix_s[...] = jnp.zeros(mix_s.shape, F32)

    def run(work):
        def score(n, ks, q0, masked):
            s = dot(k_ref[n // G, ks, :], q_ref[n, q0:, :], 1, 1)
            return jnp.where(_order(*s.shape), s, 2 * NEG) if masked else s
        def rest(s, n, ks, q0, masked):
            old = top_s[n:n+1, q0:]
            top = jnp.maximum(old, s.max(axis=0, keepdims=True))
            top_s[n:n+1, q0:] = top
            p = jnp.exp2((s - top) * e).astype(BF)
            mix_s[n, :, q0:] = mix_s[n, :, q0:] * jnp.exp2((old - top) * e) + dot(vt_s[n // G, :, ks], p)
        s = score(*work[0])
        for at, one in enumerate(work):
            after = score(*work[at + 1]) if at + 1 < len(work) else None
            rest(s, *one)
            s = after

    def full(j, _):
        run([(n, pl.ds(pl.multiple_of(j * bk, bk), bk), 0, False) for n in range(QH)])

    lax.fori_loop(0, iq * (bq // bk), full, None)
    run([(n, pl.ds(pl.multiple_of(iq * bq + k0, half), w), q0, True) for k0, w, q0 in _strips(bq, half) for n in range(QH)])
    for n in range(QH):
        total = mix_s[n, HEAD:HEAD+1, :]
        o_ref[:, n*HEAD:(n+1)*HEAD] = (mix_s[n, :HEAD, :] * (1 / total)).T.astype(BF)
        lse_ref[n:n+1, :] = top_s[n:n+1, :] * SCALE + jnp.log(total)

def attend(q, k, v, bq=1024, bk=512, half=256):
    T = q.shape[1]
    return pl.pallas_call(functools.partial(_attend, bq=bq, bk=bk, half=half), grid=(T//bq,),
        in_specs=[heads(QH, bq), whole((KVH, T, HEAD), 0, 0, 0), whole((KVH, T, HEAD), 0, 0, 0)],
        out_specs=[rows(bq, D), pl.BlockSpec((QH, bq), lambda i: (0, i))],
        out_shape=[sds((T, D)), sds((QH, T), F32)],
        scratch_shapes=[pltpu.VMEM((8, bq), F32), pltpu.VMEM((QH, HEAD+16, bq), F32), pltpu.VMEM((KVH, HEAD+16, T), BF)],
        compiler_params=params(), cost_estimate=cost(4*T*T*D, 12e6))(q, k, v)

def _attend_back(q_ref, k_ref, v_ref, do_ref, lse_ref, delta_ref, dq_ref, dk_ref, dv_ref, qt_s, dot_s, kt_s, dqt_s, dkt_s, dvt_s, *, bq, bk, half):
    iq = pl.program_id(0)
    e = SCALE * LOG2E

    @pl.when(iq == 0)
    def _():
        for i in range(KVH):
            kt_s[i] = k_ref[i].T
        dkt_s[...] = jnp.zeros(dkt_s.shape, F32)
        dvt_s[...] = jnp.zeros(dvt_s.shape, F32)

    for n in range(QH):
        qt_s[n] = q_ref[n].T
        dot_s[n] = do_ref[n].T
    dqt_s[...] = jnp.zeros(dqt_s.shape, F32)

    def run(work):
        def score(n, ks, q0, masked):
            return dot(k_ref[n // G, ks, :], q_ref[n, q0:, :], 1, 1), dot(v_ref[n // G, ks, :], do_ref[n, q0:, :], 1, 1)
        def rest(got, n, ks, q0, masked):
            s, dp = got
            i = n // G
            p = jnp.exp2(s * e - lse_ref[n:n+1, q0:] * LOG2E)
            if masked:
                p = jnp.where(_order(*p.shape), p, 0.0)
            ds = (p * (dp - delta_ref[n:n+1, q0:])).astype(BF)
            dvt_s[i, :, ks] += dot(dot_s[n, :, q0:], p.astype(BF), 1, 1)
            dkt_s[i, :, ks] += dot(qt_s[n, :, q0:], ds, 1, 1)
            dqt_s[n, :, q0:] += dot(kt_s[i, :, ks], ds, 1, 0)
        s = score(*work[0])
        for at, one in enumerate(work):
            after = score(*work[at + 1]) if at + 1 < len(work) else None
            rest(s, *one)
            s = after

    def full(j, _):
        run([(n, pl.ds(pl.multiple_of(j * bk, bk), bk), 0, False) for n in range(QH)])

    lax.fori_loop(0, iq * (bq // bk), full, None)
    run([(n, pl.ds(pl.multiple_of(iq * bq + k0, half), w), q0, True) for k0, w, q0 in _strips(bq, half) for n in range(QH)])
    for n in range(QH):
        dq_ref[n] = (dqt_s[n] * SCALE).T.astype(BF)

    @pl.when(iq == pl.num_programs(0) - 1)
    def _():
        for i in range(KVH):
            dk_ref[i] = (dkt_s[i] * SCALE).T.astype(BF)
            dv_ref[i] = dvt_s[i].T.astype(BF)

def attend_back(q, k, v, do, lse, delta, bq=512, bk=256, half=256):
    T = q.shape[1]
    stat = pl.BlockSpec((QH, bq), lambda i: (0, i))
    kvs = whole((KVH, T, HEAD), 0, 0, 0)
    return pl.pallas_call(functools.partial(_attend_back, bq=bq, bk=bk, half=half), grid=(T//bq,),
        in_specs=[heads(QH, bq), kvs, kvs, heads(QH, bq), stat, stat],
        out_specs=[heads(QH, bq), pl.BlockSpec((KVH, T, HEAD), lambda i: (0, 0, 0)), pl.BlockSpec((KVH, T, HEAD), lambda i: (0, 0, 0))],
        out_shape=[sds((QH, T, HEAD)), sds((KVH, T, HEAD)), sds((KVH, T, HEAD))],
        scratch_shapes=[pltpu.VMEM((QH, HEAD, bq), BF), pltpu.VMEM((QH, HEAD, bq), BF), pltpu.VMEM((KVH, HEAD, T), BF), pltpu.VMEM((QH, HEAD, bq), F32),
                        pltpu.VMEM((KVH, HEAD, T), F32), pltpu.VMEM((KVH, HEAD, T), F32)],
        compiler_params=params(), cost_estimate=cost(10*T*T*D, 20e6))(q, k, v, do, lse, delta)

from jax.sharding import PartitionSpec as P

THETA = 10000
NAMES = ("wq", "wk", "wv", "wo", "w_gate", "w_up", "w_down")
PEERS = 32


def _total(x_ref, o_ref, got, send_sems, recv_sems):
    me = lax.axis_index("dp")
    barrier = pltpu.get_barrier_semaphore()

    def signal(i, _):
        pl.semaphore_signal(barrier, inc=1, device_id={"dp": lax.rem(me + i, PEERS)}, device_id_type=pl.DeviceIdType.MESH)

    lax.fori_loop(1, PEERS, signal, None)
    pl.semaphore_wait(barrier, PEERS - 1)

    def copy(i, slot):
        return pltpu.make_async_remote_copy(
            src_ref=x_ref, dst_ref=got.at[slot], send_sem=send_sems.at[i], recv_sem=recv_sems.at[slot],
            device_id={"dp": lax.rem(me + i, PEERS)}, device_id_type=pl.DeviceIdType.MESH)

    lax.fori_loop(1, PEERS, lambda i, _: copy(i, me).start(), None)
    got[me] = x_ref[...]
    lax.fori_loop(1, PEERS, lambda i, _: copy(i, lax.rem(me + PEERS - i, PEERS)).wait_recv(), None)
    o_ref[...] = lax.fori_loop(1, PEERS, lambda i, so_far: so_far + got[i], got[0])
    lax.fori_loop(1, PEERS, lambda i, _: copy(i, me).wait_send(), None)


def total(x):
    x = jnp.zeros((8, 128), jnp.float32).at[0, 0].set(x)
    return pl.pallas_call(
        _total,
        out_shape=jax.ShapeDtypeStruct((8, 128), jnp.float32),
        in_specs=[pl.BlockSpec(memory_space=pltpu.VMEM)],
        out_specs=pl.BlockSpec(memory_space=pltpu.VMEM),
        scratch_shapes=[pltpu.VMEM((PEERS, 8, 128), jnp.float32), pltpu.SemaphoreType.DMA((PEERS,)), pltpu.SemaphoreType.DMA((PEERS,))],
        compiler_params=pltpu.CompilerParams(collective_id=0, has_side_effects=True),
    )(x)[0, 0]


def packed(narrow, gate, up, down):
    n = down.shape[0]
    down = down.reshape(n, 8, 8, 6, 128).transpose(0, 1, 3, 2, 4).reshape(n, 3, 16, 8, 128).transpose(0, 1, 3, 2, 4).reshape(n, 24, FF)
    return jnp.concatenate([gate, up, narrow, down], axis=1)


def unpacked(p):
    n = p.shape[0]
    down = p[:, 72:].reshape(n, 3, 8, 16, 128).transpose(0, 1, 3, 2, 4).reshape(n, 8, 6, 8, 128).transpose(0, 1, 3, 2, 4).reshape(n, 64, 768)
    return p[:, 48:72], p[:, :24], p[:, 24:48], down


def tables(tokens):
    half = HEAD // 2
    angle = jnp.arange(tokens, dtype=F32)[:, None] * THETA ** (-jnp.arange(half, dtype=F32) / half)
    c, s = jnp.cos(angle), jnp.sin(angle)
    return jnp.concatenate([c, c], 1), jnp.concatenate([-s, s], 1)


def adamw(w, m, v, g):
    m = 0.9 * m + 0.1 * g
    v = 0.95 * v + 0.05 * g * g
    step = m * lax.rsqrt(v + 1e-8) + 0.1 * w
    return (w - 0.02 * step).astype(jnp.bfloat16), m, v


def clipped(gradients, sum_of_squares, count):
    factor = jnp.minimum(1.0, 0.5 * lax.rsqrt(sum_of_squares / count + 1e-30))
    return [g * factor for g in gradients]


def solution(mesh):
    def fetched(w, number):
        mine = {name: w[name][number][None] for name in NAMES}
        narrow = jnp.concatenate([mine[name] for name in ("wq", "wo", "wk", "wv")], axis=2)
        every = lax.all_gather(packed(narrow, mine["w_gate"], mine["w_up"], mine["w_down"])[0], "dp", axis=0, tiled=True).reshape(PEERS, 96, FF)
        return tuple(one.reshape(-1, one.shape[2]) for one in unpacked(every))

    def scattered(*by_w):
        every = packed(*(one.reshape(PEERS, -1, one.shape[1]) for one in by_w))
        mine = lax.psum_scatter(every.reshape(PEERS * 96, FF), "dp", scatter_dimension=0, tiled=True)
        narrow, gate, up, down = unpacked(mine[None])
        return {"wq": narrow[:, :, :768], "wo": narrow[:, :, 768:1536], "wk": narrow[:, :, 1536:1792], "wv": narrow[:, :, 1792:],
                "w_gate": gate, "w_up": up, "w_down": down}

    def step(x, dy, *arrays):
        w, m, v = (dict(zip(NAMES, arrays[i : i + 7], strict=True)) for i in (0, 7, 14))
        layers = arrays[0].shape[0]
        whole_w = [fetched(w, number) for number in range(layers)]
        c, s = tables(x.shape[1])
        h, kept = x[0], []
        for number in range(layers):
            narrow, gate, up, down = whole_w[number]
            q, k, val = qkv(h, narrow, c, s)
            o, lse = attend(q, k, val)
            hm, g, u, out = mlp(h, o, narrow, gate, up, down)
            kept.append((h, q, k, val, o, lse, hm, g, u))
            h = out
        by_h, mine = dy[0], [None] * layers
        for number in reversed(range(layers)):
            narrow, gate, up, down = whole_w[number]
            h, q, k, val, o, lse, hm, g, u = kept[number]
            dhm, dgate, dup, prod, do, delta = mlp_back(by_h, g, u, hm, o, narrow, gate, up, down)
            by_gate, by_up, by_down = mlp_wgrad(hm, by_h, dgate, dup, prod)
            dq, dk, dv = attend_back(q, k, val, do, lse, delta)
            dqkv, by_h = qkv_back(dq, dk, dv, c, s, h, dhm, narrow)
            mine[number] = scattered(attn_wgrad(h, o, dhm, dqkv), by_gate, by_up, by_down)
        gradients = [jnp.concatenate([mine[number][name] for number in range(layers)]).astype(F32) for name in NAMES]
        squares = total(sum(jnp.sum(g * g) for g in gradients))
        gradients = clipped(gradients, squares, PEERS * sum(g.size for g in gradients))
        new = [adamw(w[name].astype(F32), m[name], v[name], g) for name, g in zip(NAMES, gradients, strict=True)]
        return tuple(one[which] for which in range(3) for one in new)

    states, cut = P(("rep", "dp"), None, None), P(None, "dp", None)
    return jax.shard_map(
        step,
        mesh=mesh,
        in_specs=(states, states) + (cut,) * 21,
        out_specs=(P("rep", "dp", None),) * 21,
        check_vma=False,
    )
```
